256 devices in a mesh: batch: 32 (over x, z), mp: 8 (over y, core).
Axes of the slice: x: 4, y: 4, z: 8, core: 2. Of those that a mesh axis runs over, the one named last changes fastest.
Arguments:
- features: bfloat16 [4096, 65536], P('batch', 'mp'), may hold values from 0 to 4
- tiles: bfloat16 [2, 512, 3, 128, 128], P(None, 'mp', None, 'batch'), may hold values from -0.3125 to 0.3125
- biases: float32 [2, 65536], P(None, 'mp'), may hold values from -0.5 to 0
- in_block: int32 [2, 512, 3], replicated, may hold values from 0 to 511, as said below
Outputs:
- activations: bfloat16 [4096, 65536], P('batch', 'mp')
- row_means: float32 [4096], P('batch')
- grand: float32 [], replicated
The draws below stay inside these ranges and needn't reach their ends.
Inputs may be any that keep to these rules, and one draw needn't show every extreme that they name: `in_block`: number the 192 tiles of mp shard m (column blocks m * 64 to (m + 1) * 64 - 1) in order of column block, then tile slot; tile number s reads a block of shard s // 24, that is an id in [(s // 24) * 64, (s // 24 + 1) * 64).
All inputs are finite; a program needn't handle non-finite values.
Results may differ from the reference program's by a relative error of at most 0.0052.
Values may be sent and summed in bfloat16 or wider, within the bound.
A program may use at most 128 MiB of HBM per device.

```python
import math
import jax
import jax.numpy as jnp
from jax import lax

NEUR = 65536
BLOCK = 128
FAN_TILES = 3
LAYERS = 2
ROWS_DEV = 128
NB = 512
CB_DEV = 64
PER_PEER = 24
ROWS = 4096


def draw_in_block(key, part):
    shard_count = NB // CB_DEV
    slots = CB_DEV * FAN_TILES
    local = jax.random.randint(key, (LAYERS, shard_count, slots), 0, CB_DEV, dtype=jnp.int32)
    source = jnp.arange(slots, dtype=jnp.int32) // PER_PEER * CB_DEV
    ids = local + source[None, None, :]
    return ids.reshape(LAYERS, NB, FAN_TILES).astype(jnp.int32)


def draw_features(key, part):
    key_scale, key_base = jax.random.split(jax.random.fold_in(key, 17))
    groups = ROWS // ROWS_DEV
    logs = jax.random.uniform(key_scale, (groups, 1, 1), jnp.float32, math.log(0.25), math.log(2.0))
    scale = jnp.exp(logs)
    base = jax.random.uniform(key_base, (groups, ROWS_DEV, NEUR), jnp.float32, 0.0, 1.0)
    base = 2.0 * base
    values = jnp.clip(scale * base, 0.0, 4.0)
    return values.reshape(ROWS, NEUR).astype(jnp.bfloat16)


def levels(rng, extent, pieces, smallest, largest):
    def one(dim, blocks):
        steps = jax.random.uniform(jax.random.fold_in(jax.random.fold_in(rng, 6), dim), (blocks,), jnp.float32, smallest / len(pieces), largest / len(pieces))
        return jnp.repeat(jnp.exp(steps), extent[dim] // blocks).reshape((-1,) + (1,) * (len(extent) - dim - 1))

    level = one(*pieces[0])
    for cut in pieces[1:]:
        level = level * one(*cut)
    return level


def gaussian(stream_key, dims, spread, most, shards=(), kind=jnp.bfloat16):
    array = jax.random.normal(stream_key, dims, jnp.float32) * spread
    if len(shards) > 0:
        array = levels(stream_key, dims, shards, -0.22, 0.18) * array
    return jnp.clip(array, min=-most, max=most).astype(kind)


def setup_inputs(seed: int = 0) -> dict:
    seeds = jax.random.split(jax.random.key(seed), 5)
    return {
        "features": draw_features(jax.random.fold_in(seeds[4], 71), 0),
        "tiles": gaussian(seeds[1], (LAYERS, NB, FAN_TILES, BLOCK, BLOCK), (FAN_TILES * BLOCK) ** -0.5, 0.3125, ((1, 8), (3, 32))),
        "biases": jnp.clip(-0.5 + 0.5 * jax.random.uniform(seeds[2], (LAYERS, NEUR), jnp.float32) ** levels(seeds[2], (LAYERS, NEUR), ((1, 8),), -0.2, 0.2), -0.5, 0.0),
        "in_block": draw_in_block(jax.random.fold_in(seeds[4], 71), 0),
    }


def one_layer(current, tile_layer, bias_layer, ids_layer):
    group = math.gcd(NB, 32)
    blocks_all = current.reshape(ROWS, NB, BLOCK)
    ids_grouped = ids_layer.reshape(NB // group, group, FAN_TILES)
    tiles_grouped = tile_layer.reshape(NB // group, group, FAN_TILES, BLOCK, BLOCK)
    bias_grouped = bias_layer.reshape(NB // group, group, BLOCK)

    def per_group(packed):
        ids_here, tiles_here, bias_here = packed
        taken = jnp.take(blocks_all, ids_here.reshape(-1), axis=1)
        taken = taken.reshape(ROWS, group, FAN_TILES, BLOCK).astype(jnp.float32)
        total = jnp.einsum("rjki,jkio->rjo", taken, tiles_here.astype(jnp.float32))
        shifted = total + bias_here[None, :, :]
        return jnp.clip(shifted, 0.0, 32.0).astype(jnp.bfloat16)

    result = lax.map(per_group, (ids_grouped, tiles_grouped, bias_grouped))
    return jnp.transpose(result, (1, 0, 2, 3)).reshape(ROWS, NEUR)


def reference(features, tiles, biases, in_block):
    current = features
    for layer_no in range(LAYERS):
        current = one_layer(current, tiles[layer_no], biases[layer_no], in_block[layer_no])
    row_means = jnp.sum(current.astype(jnp.float32), axis=1) / NEUR
    grand = jnp.sum(row_means) / ROWS
    return current, row_means, grand
```

```python
import functools

import jax
import jax.numpy as jnp
from jax import lax
from jax.experimental import pallas as pl
from jax.experimental.pallas import tpu as pltpu
from jax.sharding import PartitionSpec as P

MESH = pl.DeviceIdType.MESH
NX, NZ = 4, 8
NY, NC = 4, 2
TA = 10
LAG = 1
STAGES = 6
FAR_FIRST = ((2, 0), (2, 1), (1, 0), (3, 0), (1, 1), (3, 1), (0, 1), (0, 0))
SELF_FIRST = ((0, 0),) + FAR_FIRST[:-1]
F32 = jnp.float32
BF16 = jnp.bfloat16


def pick(j, values):
    total = 0
    for i, v in enumerate(values):
        total = total + jnp.where(j == i, v, 0)
    return total


def kernel(
    neur, rows_all,
    ib, feat, tiles, bias,
    out, means, grand,
    X0, X1, WA, WB, B, O0, O1, acc, RS, GX, GZ,
    p0s, p0r, pbs, pbr, sA, rA, sB, rB, ys, yr, rss, rsr, gxs, gxr, gzs, gzr, fsem,
):
    layers = tiles.shape[0]
    shards = tiles.shape[1]
    per_chunk = tiles.shape[2]
    cols = per_chunk // 3
    blocks = cols * shards
    chunks = layers * shards
    b = lax.axis_index("batch")
    me = lax.axis_index("mp")
    x, z = b // NZ, b % NZ
    y, c = me // NC, me % NC
    xr, xl = (x + 1) % NX, (x + NX - 1) % NX

    def zat(d):
        return (z + d + NZ) % NZ

    def at(xx, zz):
        return {"batch": xx * NZ + zz}

    right, left = at(xr, z), at(xl, z)
    up, down = at(x, zat(1)), at(x, zat(-1))

    def peer(dy, dc):
        return ((y + dy) % NY) * NC + (c + dc) % NC

    mp_peers = [peer(dy, dc) for dy, dc in FAR_FIRST[:-1]]

    def remote(src, dst, ss, rs, dev):
        return pltpu.make_async_remote_copy(
            src_ref=src, dst_ref=dst, send_sem=ss, recv_sem=rs, device_id=dev, device_id_type=MESH
        )

    def load(j, _):
        at_j = pl.ds(pl.multiple_of(j * 128, 128), 128)
        pltpu.make_async_copy(feat.at[:, at_j], X0.at[j], fsem).start()
        return 0

    barrier = pltpu.get_barrier_semaphore()
    count = 0
    for s in mp_peers:
        pl.semaphore_signal(barrier, inc=1, device_id={"mp": s}, device_id_type=MESH)
        count += 1
    for d in range(1, NX):
        pl.semaphore_signal(
            barrier, inc=1, device_id=at((x + d) % NX, z), device_id_type=MESH
        )
        count += 1
    for d in range(1, NZ):
        pl.semaphore_signal(barrier, inc=1, device_id=at(x, zat(d)), device_id_type=MESH)
        count += 1
    own = []
    for l in range(layers):
        q = l * shards + me
        own.append(
            pltpu.make_async_copy(tiles.at[l, me, 0:TA], WA.at[q, z, x], p0r.at[q, 0])
        )
        own.append(
            pltpu.make_async_copy(tiles.at[l, me, TA:per_chunk], WB.at[q, x, z], p0r.at[q, 1])
        )
    own.append(
        pltpu.make_async_copy(
            bias.at[:, pl.ds(pl.multiple_of(me * cols * 128, 128), cols * 128)],
            B.at[me],
            pbr.at[me],
        )
    )
    for copy in own:
        copy.start()
    lax.fori_loop(0, blocks, load, 0)
    pl.semaphore_wait(barrier, count)

    def part_a(l, i, s):
        q = l * shards + me
        return remote(
            tiles.at[l, s, 0:TA], WA.at[q, z, x], p0s.at[l, i, 0], p0r.at[q, 0], {"mp": s}
        )

    def part_b(l, i, s):
        q = l * shards + me
        return remote(
            tiles.at[l, s, TA:per_chunk], WB.at[q, x, z], p0s.at[l, i, 1], p0r.at[q, 1], {"mp": s}
        )

    def bias_to(i, s):
        cut = pl.ds(pl.multiple_of(s * cols * 128, 128), cols * 128)
        return remote(bias.at[:, cut], B.at[me], pbs.at[i], pbr.at[me], {"mp": s})

    order = [peer(NY - dy, dc) for dy, dc in FAR_FIRST[:-1]]
    for l in range(layers):
        for i, s in enumerate(order):
            part_a(l, i, s).start()
            part_b(l, i, s).start()
        if l == 0:
            for i, s in enumerate(order):
                bias_to(i, s).start()

    acc[...] = jnp.zeros_like(acc)

    def owner(k):
        l, j = k // shards, k % shards
        dy = jnp.where(
            l == layers - 1,
            pick(j, [d for d, _ in FAR_FIRST]),
            pick(j, [d for d, _ in SELF_FIRST]),
        )
        dc = jnp.where(
            l == layers - 1,
            pick(j, [d for _, d in FAR_FIRST]),
            pick(j, [d for _, d in SELF_FIRST]),
        )
        return l, peer(dy, dc)

    def a_copies(q, e):
        def go(ref, i, dev):
            return lambda: remote(ref, ref, sA.at[q, i], rA.at[q, i], dev)

        far_x = xl * (1 - e) + xr * e
        far_z = zat(-3) * (1 - e) + zat(3) * e
        to_x = at(xr * (1 - e) + xl * e, z)
        to_z = at(x, zat(1) * (1 - e) + zat(-1) * e)
        return [
            go(WA.at[q, z, x], 0, right),
            go(WA.at[q, z, x], 1, left),
            go(WA.at[q, z, far_x], 2, to_x),
            go(WA.at[q, z], 3, up),
            go(WA.at[q, z], 4, down),
            go(WA.at[q, zat(-1)], 5, up),
            go(WA.at[q, zat(1)], 6, down),
            go(WA.at[q, zat(-2)], 7, up),
            go(WA.at[q, zat(2)], 8, down),
            go(WA.at[q, far_z], 9, to_z),
        ]

    def b_copies(q, e):
        def go(ref, i, dev):
            return lambda: remote(ref, ref, sB.at[q, i], rB.at[q, i], dev)

        far_x = xl * (1 - e) + xr * e
        far_z = zat(3) * (1 - e) + zat(-3) * e
        to_x = at(xr * (1 - e) + xl * e, z)
        to_z = at(x, zat(-1) * (1 - e) + zat(1) * e)
        return [
            go(WB.at[q, x, z], 0, up),
            go(WB.at[q, x, z], 1, down),
            go(WB.at[q, x, zat(-1)], 2, up),
            go(WB.at[q, x, zat(1)], 3, down),
            go(WB.at[q, x, zat(-2)], 4, up),
            go(WB.at[q, x, zat(2)], 5, down),
            go(WB.at[q, x, far_z], 6, to_z),
            go(WB.at[q, x], 7, right),
            go(WB.at[q, x], 8, left),
            go(WB.at[q, far_x], 9, to_x),
        ]


    def stage(h, k):
        l, m = owner(k)
        q = l * shards + m
        e = k % 2
        a, bb = a_copies(q, e), b_copies(q, e)
        if h == 0:
            pltpu.make_async_copy(WA.at[q, z, x], WA.at[q, z, x], p0r.at[q, 0]).wait()
            a[0]().start()
            a[1]().start()
            pltpu.make_async_copy(WB.at[q, x, z], WB.at[q, x, z], p0r.at[q, 1]).wait()
            bb[0]().start()
            bb[1]().start()
        elif h == 1:
            a[0]().wait_recv()
            a[1]().wait_recv()
            a[2]().start()
            bb[0]().wait_recv()
            bb[2]().start()
            bb[1]().wait_recv()
            bb[3]().start()
        elif h == 2:
            a[2]().wait_recv()
            a[3]().start()
            a[4]().start()
            bb[2]().wait_recv()
            bb[4]().start()
            bb[3]().wait_recv()
            bb[5]().start()
        elif h == 3:
            a[3]().wait_recv()
            a[5]().start()
            a[4]().wait_recv()
            a[6]().start()
            bb[4]().wait_recv()
            bb[5]().wait_recv()
            bb[6]().start()
        elif h == 4:
            a[5]().wait_recv()
            a[7]().start()
            a[6]().wait_recv()
            a[8]().start()
            bb[6]().wait_recv()
            bb[7]().start()
            bb[8]().start()
        elif h == 5:
            a[7]().wait_recv()
            a[8]().wait_recv()
            a[9]().start()
            bb[7]().wait_recv()
            bb[8]().wait_recv()
            bb[9]().start()
        else:
            a[9]().wait_recv()
            bb[9]().wait_recv()

    mine = pl.ds(me * cols, cols)
    mine_out = pl.ds(pl.multiple_of(me * cols * 128, 128), cols * 128)

    def y_copy(l, m):
        if l == 0:
            src, dst = O0.at[m], X1.at[mine]
        else:
            src, dst = O1.at[m], out.at[:, mine_out]
        return remote(src, dst, ys.at[l, m], yr.at[l, me], {"mp": m})

    def y_arrival(l, s):
        if l == 0:
            src, dst = O0.at[s], X1.at[pl.ds(s * cols, cols)]
        else:
            cut = pl.ds(pl.multiple_of(s * cols * 128, 128), cols * 128)
            src, dst = O1.at[s], out.at[:, cut]
        remote(src, dst, ys.at[l, s], yr.at[l, s], {"mp": s}).wait_recv()

    def compute(l, k):
        _, m = owner(k)
        q = l * shards + m
        source = X0 if l == 0 else X1
        if l == 0:

            @pl.when(k == 0)
            def _():
                pltpu.make_async_copy(X0, X0, fsem).wait()

            pltpu.make_async_copy(B.at[m], B.at[m], pbr.at[m]).wait()
        else:

            @pl.when(k == shards)
            def _():
                for s in mp_peers:
                    y_arrival(0, s)

        for j in range(cols):
            total = None
            for t in range(3):
                f = 3 * j + t
                block = lax.rem(ib[t, l, m * blocks + me * cols + j], blocks)
                lhs = source[block]
                if f < TA:
                    w = jnp.transpose(WA[q, :, :, f], (1, 0, 2, 3)).reshape(128, 128)
                else:
                    w = WB[q, :, :, f - TA].reshape(128, 128)
                d = jnp.dot(lhs, w, preferred_element_type=F32)
                total = d if total is None else total + d
            row = B[m, l : l + 1, j * 128 : (j + 1) * 128]
            value = jnp.clip(total + row, 0.0, 32.0).astype(BF16)
            if l == 0:
                O0[m, j] = value
            else:
                O1[m, :, j * 128 : (j + 1) * 128] = value
                acc[...] += value.astype(F32)

        @pl.when(m == me)
        def _():
            if l == 0:
                X1[mine] = O0[m]
            else:
                out[:, mine_out] = O1[m]

        @pl.when(m != me)
        def _():
            y_copy(l, m).start()

    def step(i, _):
        for h in range(STAGES, -1, -1):
            k = i - h

            @pl.when(jnp.logical_and(k >= 0, k < chunks))
            def _():
                stage(h, k)

        first = i - STAGES

        @pl.when(jnp.logical_and(first >= 0, first < shards))
        def _():
            compute(0, first)

        second = first - LAG

        @pl.when(second >= shards)
        def _():
            compute(1, second)

        return 0

    lax.fori_loop(0, chunks + STAGES + LAG, step, 0)

    part = jnp.sum(acc[...].T, axis=0, keepdims=True)
    RS[me] = jnp.broadcast_to(part, (8, 128))
    rs_copies = [
        remote(RS.at[me], RS.at[me], rss.at[i], rsr.at[me], {"mp": s})
        for i, s in enumerate(mp_peers)
    ]
    for copy in rs_copies:
        copy.start()

    for i, s in enumerate(mp_peers):
        remote(RS.at[s], RS.at[s], rss.at[i], rsr.at[s], {"mp": s}).wait_recv()
    row = RS[0, 0:1]
    for s in range(1, shards):
        row = row + RS[s, 0:1]
    row = row / neur
    means[...] = row
    GX[x] = jnp.broadcast_to(jnp.sum(row, axis=1, keepdims=True), (8, 128))
    gx_copies = [
        remote(GX.at[x], GX.at[x], gxs.at[d], gxr.at[x], at((x + d) % NX, z))
        for d in range(1, NX)
    ]
    for copy in gx_copies:
        copy.start()
    for d in range(1, NX):
        n = (x + d) % NX
        remote(GX.at[n], GX.at[n], gxs.at[d], gxr.at[n], at(n, z)).wait_recv()
    GZ[z] = GX[0] + GX[1] + GX[2] + GX[3]
    gz_copies = [
        remote(GZ.at[z], GZ.at[z], gzs.at[d], gzr.at[z], at(x, zat(d))) for d in range(1, NZ)
    ]
    for copy in gz_copies:
        copy.start()
    for d in range(1, NZ):
        n = zat(d)
        remote(GZ.at[n], GZ.at[n], gzs.at[d], gzr.at[n], at(x, n)).wait_recv()
    total = GZ[0, 0:1]
    for n in range(1, NZ):
        total = total + GZ[n, 0:1]
    grand[...] = total / rows_all

    for s in mp_peers:
        y_arrival(1, s)

    def drain(k, _):
        for copy in a_copies(k, 0) + b_copies(k, 0):
            copy().wait_send()
        return 0

    lax.fori_loop(0, chunks, drain, 0)
    for l in range(layers):
        for i, s in enumerate(order):
            part_a(l, i, s).wait_send()
            part_b(l, i, s).wait_send()
        for s in mp_peers:
            y_copy(l, s).wait_send()
    for i, s in enumerate(order):
        bias_to(i, s).wait_send()
    for copy in rs_copies + gx_copies + gz_copies:
        copy.wait_send()


def on_device(features, tiles, biases, in_block):
    layers, cb, fan, own_rows, side = tiles.shape
    rows = features.shape[0]
    shards = lax.axis_size("mp")
    groups = lax.axis_size("batch")
    per_chunk = cb // shards * fan
    chunks = layers * shards
    vmem = pl.BlockSpec(memory_space=pltpu.VMEM)
    any_ = pl.BlockSpec(memory_space=pl.ANY)
    dma = pltpu.SemaphoreType.DMA
    current, means, grand = pl.pallas_call(
        functools.partial(kernel, cb * shards * side, rows * groups),
        out_shape=(
            jax.ShapeDtypeStruct((rows, cb * side), BF16),
            jax.ShapeDtypeStruct((1, rows), F32),
            jax.ShapeDtypeStruct((1, 128), F32),
        ),
        in_specs=[pl.BlockSpec(memory_space=pltpu.SMEM), any_, vmem, vmem],
        out_specs=(vmem, vmem, vmem),
        scratch_shapes=[
            pltpu.VMEM((cb, rows, side), BF16),
            pltpu.VMEM((cb, rows, side), BF16),
            pltpu.VMEM((chunks, NZ, NX, TA, own_rows, side), BF16),
            pltpu.VMEM((chunks, NX, NZ, per_chunk - TA, own_rows, side), BF16),
            pltpu.VMEM((shards, layers, cb // shards * side), F32),
            pltpu.VMEM((shards, cb // shards, rows, side), BF16),
            pltpu.VMEM((shards, rows, cb // shards * side), BF16),
            pltpu.VMEM((rows, side), F32),
            pltpu.VMEM((shards, 8, 128), F32),
            pltpu.VMEM((NX, 8, 128), F32),
            pltpu.VMEM((NZ, 8, 128), F32),
            dma((layers, shards - 1, 2)),
            dma((chunks, 2)),
            dma((shards - 1,)),
            dma((shards,)),
            dma((chunks, 10)),
            dma((chunks, 10)),
            dma((chunks, 10)),
            dma((chunks, 10)),
            dma((layers, shards)),
            dma((layers, shards)),
            dma((shards - 1,)),
            dma((shards,)),
            dma((NX,)),
            dma((NX,)),
            dma((NZ,)),
            dma((NZ,)),
            dma,
        ],
        compiler_params=pltpu.CompilerParams(
            collective_id=0, has_side_effects=True, vmem_limit_bytes=48 * 1024 * 1024
        ),
    )(
        jnp.transpose(in_block, (2, 0, 1)),
        features,
        tiles.reshape(layers, shards, per_chunk, own_rows, side),
        biases,
    )
    return current, means.reshape(rows), grand[0, 0]


def solution(mesh):
    placed = (P("batch", "mp"), P(None, "mp", None, "batch", None), P(None, "mp"), P())
    return jax.shard_map(
        on_device,
        mesh=mesh,
        in_specs=placed,
        out_specs=(P("batch", "mp"), P("batch"), P()),
        check_vma=False,
    )
```

```python
import functools

import jax
import jax.numpy as jnp
from jax import lax
from jax.experimental import pallas as pl
from jax.experimental.pallas import tpu as pltpu
from jax.sharding import PartitionSpec as P

NX, NZ = 4, 8
NY, NC = 4, 2
TA = 10
LAGS_A = (0, 1, 2, 3, 4, 5, 6)
LAGS_B = (0, 1, 2, 3, 4, 5, 6)
LAG = 1
F32 = jnp.float32
BF16 = jnp.bfloat16


def kernel(
    neur, rows_all,
    ib, feat, tiles, bias,
    out, means, grand,
    X0, X1, WA, WB, B, O0, O1, acc, RS, G, ids,
    p0s, p0r, pbs, pbr, sA, rA, sB, rB, ys, yr, rss, rsr, gs, gr, fsem, isem,
):
    layers = tiles.shape[0]
    shards = tiles.shape[1]
    per_chunk = tiles.shape[2]
    cols = per_chunk // 3
    blocks = cols * shards
    chunks = layers * shards
    b = lax.axis_index("batch")
    me = lax.axis_index("mp")
    x, z = b // NZ, b % NZ
    y, c = me // NC, me % NC
    xr, xl = (x + 1) % NX, (x + NX - 1) % NX

    def zat(d):
        return (z + d + NZ) % NZ

    def device(xx, zz, s):
        return (xx * NZ + zz) * shards + s

    near = {d: zat(d) for d in range(-3, 4)}
    right, left = device(xr, z, me), device(xl, z, me)
    up, down = device(x, near[1], me), device(x, near[-1], me)

    def peer(dy, dc):
        return lax.rem(y + dy, NY) * NC + lax.rem(c + dc, NC)

    def mate(s):
        return device(x, z, s)

    offsets = [(2, 0), (2, 1), (1, 0), (3, 0), (1, 1), (3, 1), (0, 1)]
    mp_peers = [peer(dy, dc) for dy, dc in offsets]

    def remote(src, dst, ss, rs, dev):
        return pltpu.make_async_remote_copy(
            src_ref=src,
            dst_ref=dst,
            send_sem=ss,
            recv_sem=rs,
            device_id=dev,
            device_id_type=pl.DeviceIdType.LOGICAL,
        )

    def load(j, _):
        at_j = pl.ds(pl.multiple_of(j * 128, 128), 128)
        pltpu.make_async_copy(feat.at[:, at_j], X0.at[j], fsem).start()
        return 0

    barrier = pltpu.get_barrier_semaphore()
    greeted = [mate(s) for s in mp_peers] + [right, left, up, down]
    for dev in greeted:
        pl.semaphore_signal(
            barrier, inc=1, device_id=dev, device_id_type=pl.DeviceIdType.LOGICAL
        )
    own = []
    for l in range(layers):
        q = l * shards + me
        own.append(
            pltpu.make_async_copy(tiles.at[l, me, 0:TA], WA.at[q, z, x], p0r.at[q, 0])
        )
        own.append(
            pltpu.make_async_copy(tiles.at[l, me, TA:per_chunk], WB.at[q, x, z], p0r.at[q, 1])
        )
    own.append(
        pltpu.make_async_copy(
            bias.at[:, pl.ds(pl.multiple_of(me * cols * 128, 128), cols * 128)],
            B.at[me],
            pbr.at[me],
        )
    )
    for copy in own:
        copy.start()
    pltpu.make_async_copy(ib, ids, isem).start()
    lax.fori_loop(0, blocks, load, 0)
    pl.semaphore_wait(barrier, len(greeted))

    def part_a(l, i, s):
        q = l * shards + me
        return remote(
            tiles.at[l, s, 0:TA], WA.at[q, z, x], p0s.at[l, i, 0], p0r.at[q, 0], mate(s)
        )

    def part_b(l, i, s):
        q = l * shards + me
        return remote(
            tiles.at[l, s, TA:per_chunk], WB.at[q, x, z], p0s.at[l, i, 1], p0r.at[q, 1], mate(s)
        )

    def bias_to(i, s):
        cut = pl.ds(pl.multiple_of(s * cols * 128, 128), cols * 128)
        return remote(bias.at[:, cut], B.at[me], pbs.at[i], pbr.at[me], mate(s))

    order = [peer(NY - dy, dc) for dy, dc in offsets]
    for l in range(layers):
        for i in range(shards - 1):
            part_a(l, i, order[i]).start()
            part_b(l, i, order[i]).start()
        if l == 0:
            for i, s in enumerate(order):
                bias_to(i, s).start()

    acc[...] = jnp.zeros_like(acc)

    def owner(k):
        l = jnp.where(k >= shards, 1, 0)
        n = lax.rem(k + (1 - l) * (shards - 1), shards)
        dy = jnp.where(n < 2, 2, jnp.where(n < 6, 1 + 2 * lax.rem(n, 2), 0))
        dc = jnp.where(n < 2, n, jnp.where(n < 6, lax.div(n - 2, 2), 7 - n))
        return l, peer(dy, dc)

    def a_copies(q):
        def go(ref, i, dev):
            return lambda: remote(ref, ref, sA.at[q, i], rA.at[q, i], dev)

        half, cut = NX // 2, TA // 2
        return [
            go(WA.at[q, z, x], 0, right),
            go(WA.at[q, z, x], 1, left),
            go(WA.at[q, z, xl, 0:cut], 2, right),
            go(WA.at[q, z, xr, cut:TA], 3, left),
            go(WA.at[q, z], 4, up),
            go(WA.at[q, z], 5, down),
            go(WA.at[q, near[-1]], 6, up),
            go(WA.at[q, near[1]], 7, down),
            go(WA.at[q, near[-2]], 8, up),
            go(WA.at[q, near[2]], 9, down),
            go(WA.at[q, near[-3], 0:half], 10, up),
            go(WA.at[q, near[3], half:NX], 11, down),
        ]

    def b_copies(q):
        def go(ref, i, dev):
            return lambda: remote(ref, ref, sB.at[q, i], rB.at[q, i], dev)

        tb = per_chunk - TA
        half, cut = NZ // 2, tb // 2
        return [
            go(WB.at[q, x, z], 0, up),
            go(WB.at[q, x, z], 1, down),
            go(WB.at[q, x, near[-1]], 2, up),
            go(WB.at[q, x, near[1]], 3, down),
            go(WB.at[q, x, near[-2]], 4, up),
            go(WB.at[q, x, near[2]], 5, down),
            go(WB.at[q, x, near[-3], 0:cut], 6, up),
            go(WB.at[q, x, near[3], cut:tb], 7, down),
            go(WB.at[q, x], 8, right),
            go(WB.at[q, x], 9, left),
            go(WB.at[q, xl, 0:half], 10, right),
            go(WB.at[q, xr, half:NZ], 11, left),
        ]

    def stage_a(h, q):
        copies = a_copies(q)

        def forward(needs, starts):
            for n in needs:
                copies[n]().wait_recv()
            for n in starts:
                copies[n]().start()

        if h == 0:
            pltpu.make_async_copy(WA.at[q, z, x], WA.at[q, z, x], p0r.at[q, 0]).wait()
            forward((), (0, 1))
        elif h == 1:
            forward((0,), (2,))
            forward((1,), (3,))
        elif h == 2:
            forward((2, 3), (4, 5))
        elif h < 6:
            forward((2 * h - 2,), (2 * h,))
            forward((2 * h - 1,), (2 * h + 1,))
        else:
            forward((10, 11), ())

    def stage_b(h, q):
        copies = b_copies(q)

        def forward(needs, starts):
            for n in needs:
                copies[n]().wait_recv()
            for n in starts:
                copies[n]().start()

        if h == 0:
            pltpu.make_async_copy(WB.at[q, x, z], WB.at[q, x, z], p0r.at[q, 1]).wait()
            forward((), (0, 1))
        elif h == 4:
            forward((6, 7), (8, 9))
        elif h < 6:
            forward((2 * h - 2,), (2 * h,))
            forward((2 * h - 1,), (2 * h + 1,))
        else:
            forward((10, 11), ())

    mine = pl.ds(me * cols, cols)
    mine_out = pl.ds(pl.multiple_of(me * cols * 128, 128), cols * 128)

    def y_copy(l, m):
        if l == 0:
            src, dst = O0.at[m], X1.at[mine]
        else:
            src, dst = O1.at[m], out.at[:, mine_out]
        return remote(src, dst, ys.at[l, m], yr.at[l, me], mate(m))

    def y_arrival(l, s):
        if l == 0:
            src, dst = O0.at[s], X1.at[pl.ds(s * cols, cols)]
        else:
            cut = pl.ds(pl.multiple_of(s * cols * 128, 128), cols * 128)
            src, dst = O1.at[s], out.at[:, cut]
        remote(src, dst, ys.at[l, s], yr.at[l, s], mate(s)).wait_recv()

    def compute(l, k):
        _, m = owner(k)
        q = l * shards + m
        source = X0 if l == 0 else X1
        if l == 0:

            @pl.when(k == 0)
            def _():
                pltpu.make_async_copy(X0, X0, fsem).wait()
                pltpu.make_async_copy(ib, ids, isem).wait()

            pltpu.make_async_copy(B.at[m], B.at[m], pbr.at[m]).wait()
        else:

            @pl.when(k == shards)
            def _():
                for s in mp_peers:
                    y_arrival(0, s)

        for j in range(cols):
            total = None
            for t in range(3):
                f = 3 * j + t
                block = lax.rem(ids[t, l, m * blocks + me * cols + j], blocks)
                lhs = source[block]
                if f < TA:
                    w = jnp.transpose(WA[q, :, :, f], (1, 0, 2, 3)).reshape(128, 128)
                else:
                    w = WB[q, :, :, f - TA].reshape(128, 128)
                d = jnp.dot(lhs, w, preferred_element_type=F32)
                total = d if total is None else total + d
            row = B[m, l : l + 1, j * 128 : (j + 1) * 128]
            value = jnp.clip(total + row, 0.0, 32.0).astype(BF16)
            if l == 0:
                O0[m, j] = value
            else:
                O1[m, :, j * 128 : (j + 1) * 128] = value
                acc[...] += value.astype(F32)

        @pl.when(m == me)
        def _():
            if l == 0:
                X1[mine] = O0[m]
            else:
                out[:, mine_out] = O1[m]

        @pl.when(m != me)
        def _():
            y_copy(l, m).start()

    def ring_steps(i, h):
        for stage, lags in ((stage_b, LAGS_B), (stage_a, LAGS_A)):
            k = i - lags[h]

            @pl.when(jnp.logical_and(k >= 0, k < chunks))
            def _():
                l, m = owner(k)
                stage(h, l * shards + m)

    done = max(LAGS_A[-1], LAGS_B[-1])

    def step(i, _):
        for h in range(7):
            ring_steps(i, h)

        first = i - done

        @pl.when(jnp.logical_and(first >= 0, first < shards))
        def _():
            compute(0, first)

        second = first - LAG

        @pl.when(second >= shards)
        def _():
            compute(1, second)

        return 0

    lax.fori_loop(0, chunks + done + LAG, step, 0)

    part = jnp.sum(acc[...].T, axis=0, keepdims=True)
    RS[me] = part
    rs_copies = [
        remote(RS.at[me], RS.at[me], rss.at[i], rsr.at[me], mate(s)) for i, s in enumerate(mp_peers)
    ]
    for copy in rs_copies:
        copy.start()

    for i, s in enumerate(mp_peers):
        remote(RS.at[s], RS.at[s], rss.at[i], rsr.at[s], mate(s)).wait_recv()
    row = jnp.sum(RS[...], axis=0) / neur
    means[...] = row
    G[b] = jnp.broadcast_to(jnp.sum(row, axis=1, keepdims=True), (1, 128))

    def tell(d, _):
        to = lax.rem(b + d, NX * NZ) * shards + me
        remote(G.at[b], G.at[b], gs, gr, to).start()
        return 0

    lax.fori_loop(1, NX * NZ, tell, 0)
    others = G.at[pl.ds(0, NX * NZ - 1)]
    pltpu.make_async_copy(others, others, gr).wait()
    grand[...] = jnp.sum(G[...], axis=0) / rows_all
    for s in mp_peers:
        y_arrival(1, s)

    def drain(k, _):
        for copy in a_copies(k) + b_copies(k):
            copy().wait_send()
        return 0

    lax.fori_loop(0, chunks, drain, 0)
    for l in range(layers):
        for i, s in enumerate(order):
            part_a(l, i, s).wait_send()
            part_b(l, i, s).wait_send()
        for s in mp_peers:
            y_copy(l, s).wait_send()
    for i, s in enumerate(order):
        bias_to(i, s).wait_send()
    for copy in rs_copies:
        copy.wait_send()
    pltpu.make_async_copy(others, others, gs).wait()


def on_device(features, tiles, biases, in_block):
    layers, cb, fan, own_rows, side = tiles.shape
    rows = features.shape[0]
    shards = lax.axis_size("mp")
    groups = lax.axis_size("batch")
    per_chunk = cb // shards * fan
    chunks = layers * shards
    vmem = pl.BlockSpec(memory_space=pltpu.VMEM)
    hbm = pl.BlockSpec(memory_space=pltpu.HBM)
    dma = pltpu.SemaphoreType.DMA
    current, means, grand = pl.pallas_call(
        functools.partial(kernel, cb * shards * side, rows * groups),
        out_shape=(
            jax.ShapeDtypeStruct((rows, cb * side), BF16),
            jax.ShapeDtypeStruct((1, rows), F32),
            jax.ShapeDtypeStruct((1, 128), F32),
        ),
        in_specs=[hbm, hbm, hbm, hbm],
        out_specs=(vmem, vmem, vmem),
        scratch_shapes=[
            pltpu.VMEM((cb, rows, side), BF16),
            pltpu.VMEM((cb, rows, side), BF16),
            pltpu.VMEM((chunks, NZ, NX, TA, own_rows, side), BF16),
            pltpu.VMEM((chunks, NX, NZ, per_chunk - TA, own_rows, side), BF16),
            pltpu.VMEM((shards, layers, cb // shards * side), F32),
            pltpu.VMEM((shards, cb // shards, rows, side), BF16),
            pltpu.VMEM((shards, rows, cb // shards * side), BF16),
            pltpu.VMEM((rows, side), F32),
            pltpu.VMEM((shards, 1, 128), F32),
            pltpu.VMEM((NX * NZ, 1, 128), F32),
            pltpu.SMEM((fan, layers, shards * cb), jnp.int32),
            dma((layers, shards - 1, 2)),
            dma((chunks, 2)),
            dma((shards - 1,)),
            dma((shards,)),
            dma((chunks, 12)),
            dma((chunks, 12)),
            dma((chunks, 12)),
            dma((chunks, 12)),
            dma((layers, shards)),
            dma((layers, shards)),
            dma((shards - 1,)),
            dma((shards,)),
            dma,
            dma,
            dma,
            dma,
        ],
        compiler_params=pltpu.CompilerParams(
            collective_id=0, has_side_effects=True, vmem_limit_bytes=67043328
        ),
    )(
        jnp.transpose(in_block, (2, 0, 1)),
        features,
        tiles.reshape(layers, shards, per_chunk, own_rows, side),
        biases,
    )
    return current, means.reshape(rows), grand[0, 0]


def solution(mesh):
    placed = (P("batch", "mp"), P(None, "mp", None, "batch", None), P(None, "mp"), P())
    return jax.shard_map(
        on_device,
        mesh=mesh,
        in_specs=placed,
        out_specs=(P("batch", "mp"), P("batch"), P()),
        check_vma=False,
    )
```

```python
import functools

import jax
import jax.numpy as jnp
from jax import lax
from jax.experimental import pallas as pl
from jax.experimental.pallas import tpu as pltpu
from jax.sharding import PartitionSpec as P

NX, NZ = 4, 8
NY, NC = 4, 2
TA = 10
LAGS_A = (0, 1, 2, 3, 4, 5, 6)
LAGS_B = (0, 1, 2, 3, 4, 5, 6)
HEAD = 0
F32 = jnp.float32
BF16 = jnp.bfloat16


def kernel(
    neur, rows_all,
    ib, feat, tiles, bias,
    out, means, grand,
    X0, X1, WA, WB, B, O0, O1, acc, RS, G, ids,
    p0s, p0r, pbs, pbr, sA, rA, sB, rB, ys, yr, rss, rsr, gs, gr, fsem, isem, osem,
):
    layers = tiles.shape[0]
    shards = tiles.shape[1]
    per_chunk = tiles.shape[2]
    cols = per_chunk // 3
    blocks = cols * shards
    chunks = layers * shards
    b = lax.axis_index("batch")
    me = lax.axis_index("mp")
    x, z = b // NZ, b % NZ
    y, c = me // NC, me % NC
    xr, xl = (x + 1) % NX, (x + NX - 1) % NX

    def zat(d):
        return (z + d + NZ) % NZ

    def device(xx, zz, s):
        return (xx * NZ + zz) * shards + s

    near = {d: zat(d) for d in range(-3, NZ // 2 + 1)}
    right, left = device(xr, z, me), device(xl, z, me)
    up, down = device(x, near[1], me), device(x, near[-1], me)

    def peer(dy, dc):
        return lax.rem(y + dy, NY) * NC + lax.rem(c + dc, NC)

    def mate(s):
        return device(x, z, s)

    offsets = [(2, 0), (2, 1), (1, 0), (3, 0), (1, 1), (3, 1), (0, 1)]
    mp_peers = [peer(dy, dc) for dy, dc in offsets]

    def remote(src, dst, ss, rs, dev):
        return pltpu.make_async_remote_copy(
            src_ref=src,
            dst_ref=dst,
            send_sem=ss,
            recv_sem=rs,
            device_id=dev,
            device_id_type=pl.DeviceIdType.LOGICAL,
        )

    def load(j, _):
        at_j = pl.ds(pl.multiple_of(j * 128, 128), 128)
        pltpu.make_async_copy(feat.at[:, at_j], X0.at[j], fsem).start()
        return 0

    barrier = pltpu.get_barrier_semaphore()
    across = device(lax.rem(x + NX // 2, NX), z, me)
    beyond = {d: device(x, near[d], me) for d in near if d != 0}
    greeted = [mate(s) for s in mp_peers] + [right, left, up, down]
    for dev in greeted:
        pl.semaphore_signal(
            barrier, inc=1, device_id=dev, device_id_type=pl.DeviceIdType.LOGICAL
        )
    own = []
    for l in range(layers):
        q = l * shards + me
        own.append(
            pltpu.make_async_copy(tiles.at[l, me, 0:TA], WA.at[q, z, x], p0r.at[q, 0])
        )
        own.append(
            pltpu.make_async_copy(tiles.at[l, me, TA:per_chunk], WB.at[q, x, z], p0r.at[q, 1])
        )
    own.append(
        pltpu.make_async_copy(
            bias.at[:, pl.ds(pl.multiple_of(me * cols * 128, 128), cols * 128)],
            B.at[me],
            pbr.at[me],
        )
    )
    for copy in own:
        copy.start()
    pltpu.make_async_copy(ib, ids, isem).start()
    lax.fori_loop(0, blocks, load, 0)
    pl.semaphore_wait(barrier, len(greeted))

    def part_a(l, i, s):
        q = l * shards + me
        return remote(
            tiles.at[l, s, 0:TA], WA.at[q, z, x], p0s.at[l, i, 0], p0r.at[q, 0], mate(s)
        )

    def part_b(l, i, s):
        q = l * shards + me
        return remote(
            tiles.at[l, s, TA:per_chunk], WB.at[q, x, z], p0s.at[l, i, 1], p0r.at[q, 1], mate(s)
        )

    def bias_to(i, s):
        cut = pl.ds(pl.multiple_of(s * cols * 128, 128), cols * 128)
        return remote(bias.at[:, cut], B.at[me], pbs.at[i], pbr.at[me], mate(s))

    order = [peer(NY - dy, dc) for dy, dc in offsets]
    for l in range(layers):
        for i in range(shards - 1):
            part_a(l, i, order[i]).start()
            part_b(l, i, order[i]).start()
        if l == 0:
            for i, s in enumerate(order):
                bias_to(i, s).start()

    acc[...] = jnp.zeros_like(acc)

    def owner(k):
        tail = k >= shards + 1
        l = jnp.where(jnp.logical_or(k == 1, tail), 1, 0)
        n = jnp.where(k < 2, shards - 1, jnp.where(tail, k - (shards + 1), k - 2))
        dy = jnp.where(n < 2, 2, jnp.where(n < 6, 1 + 2 * lax.rem(n, 2), 0))
        dc = jnp.where(n < 2, n, jnp.where(n < 6, lax.div(n - 2, 2), 7 - n))
        return l, peer(dy, dc)

    def a_copies(q):
        def go(ref, i, dev):
            return lambda: remote(ref, ref, sA.at[q, i], rA.at[q, i], dev)

        half, cut = NX // 2, TA // 2
        return [
            go(WA.at[q, z, x], 0, right),
            go(WA.at[q, z, x], 1, left),
            go(WA.at[q, z, xl, 0:cut], 2, right),
            go(WA.at[q, z, xr, cut:TA], 3, left),
            go(WA.at[q, z], 4, up),
            go(WA.at[q, z], 5, down),
            go(WA.at[q, near[-1]], 6, up),
            go(WA.at[q, near[1]], 7, down),
            go(WA.at[q, near[-2]], 8, up),
            go(WA.at[q, near[2]], 9, down),
            go(WA.at[q, near[-3], 0:half], 10, up),
            go(WA.at[q, near[3], half:NX], 11, down),
        ]

    def b_copies(q):
        def go(ref, i, dev):
            return lambda: remote(ref, ref, sB.at[q, i], rB.at[q, i], dev)

        tb = per_chunk - TA
        half, cut = NZ // 2, tb // 2
        return [
            go(WB.at[q, x, z], 0, up),
            go(WB.at[q, x, z], 1, down),
            go(WB.at[q, x, near[-1]], 2, up),
            go(WB.at[q, x, near[1]], 3, down),
            go(WB.at[q, x, near[-2]], 4, up),
            go(WB.at[q, x, near[2]], 5, down),
            go(WB.at[q, x, near[-3], 0:cut], 6, up),
            go(WB.at[q, x, near[3], cut:tb], 7, down),
            go(WB.at[q, x], 8, right),
            go(WB.at[q, x], 9, left),
            go(WB.at[q, xl, 0:half], 10, right),
            go(WB.at[q, xr, half:NZ], 11, left),
        ]

    def stage_a(h, k, q):
        copies = a_copies(q)

        def forward(needs, starts):
            for n in needs:
                copies[n]().wait_recv()
            for n in starts:
                copies[n]().start()

        if h == 0:
            pltpu.make_async_copy(WA.at[q, z, x], WA.at[q, z, x], p0r.at[q, 0]).wait()
            forward((), (0, 1))
        elif h == 1:
            forward((0,), (2,))
            forward((1,), (3,))
        elif h == 2:

            @pl.when(k < HEAD)
            def _():
                forward((0, 1), ())

            forward((2, 3), (4, 5))
        elif h < 6:
            forward((2 * h - 2,), (2 * h,))
            forward((2 * h - 1,), (2 * h + 1,))
        else:
            forward((10, 11), ())

    def stage_b(h, k, q):
        copies = b_copies(q)

        def forward(needs, starts):
            for n in needs:
                copies[n]().wait_recv()
            for n in starts:
                copies[n]().start()

        if h == 0:
            pltpu.make_async_copy(WB.at[q, x, z], WB.at[q, x, z], p0r.at[q, 1]).wait()
            forward((), (0, 1))
        elif h == 4:

            @pl.when(k < HEAD)
            def _():
                forward(range(6), ())

            forward((6, 7), (8, 9))
        elif h < 6:
            forward((2 * h - 2,), (2 * h,))
            forward((2 * h - 1,), (2 * h + 1,))
        else:
            forward((10, 11), ())

    def head(k):
        l, m = owner(k)
        q = l * shards + m
        tb = per_chunk - TA
        cut_a, cut_b = TA // 2, tb // 2

        def go_a(ref, i, dev):
            remote(ref, ref, sA.at[q, i], rA.at[q, i], dev).start()

        def go_b(ref, i, dev):
            remote(ref, ref, sB.at[q, i], rB.at[q, i], dev).start()

        pltpu.make_async_copy(WB.at[q, x, z], WB.at[q, x, z], p0r.at[q, 1]).wait()
        for d in range(NZ // 2 - 1, 0, -1):
            go_b(WB.at[q, x, z], 2 * d - 2, beyond[d])
            go_b(WB.at[q, x, z], 2 * d - 1, beyond[-d])
        go_b(WB.at[q, x, z, 0:cut_b], 6, beyond[NZ // 2])
        go_b(WB.at[q, x, z, cut_b:tb], 7, beyond[NZ // 2])
        pltpu.make_async_copy(WA.at[q, z, x], WA.at[q, z, x], p0r.at[q, 0]).wait()
        go_a(WA.at[q, z, x, 0:cut_a], 2, across)
        go_a(WA.at[q, z, x, cut_a:TA], 3, across)
        go_a(WA.at[q, z, x], 0, right)
        go_a(WA.at[q, z, x], 1, left)

    mine = pl.ds(me * cols, cols)
    mine_out = pl.ds(pl.multiple_of(me * cols * 128, 128), cols * 128)

    def y_copy(l, m):
        if l == 0:
            src, dst = O0.at[m], X1.at[mine]
        else:
            src, dst = O1.at[m], out.at[:, mine_out]
        return remote(src, dst, ys.at[l, m], yr.at[l, me], mate(m))

    def y_arrival(l, s):
        if l == 0:
            src, dst = O0.at[s], X1.at[pl.ds(s * cols, cols)]
        else:
            cut = pl.ds(pl.multiple_of(s * cols * 128, 128), cols * 128)
            src, dst = O1.at[s], out.at[:, cut]
        remote(src, dst, ys.at[l, s], yr.at[l, s], mate(s)).wait_recv()

    def compute(l, k):
        _, m = owner(k)
        q = l * shards + m
        source = X0 if l == 0 else X1
        if l == 0:

            @pl.when(k == 0)
            def _():
                pltpu.make_async_copy(X0, X0, fsem).wait()
                pltpu.make_async_copy(ib, ids, isem).wait()

            pltpu.make_async_copy(B.at[m], B.at[m], pbr.at[m]).wait()
        else:

            @pl.when(k == 1)
            def _():
                for s in mp_peers:
                    y_arrival(0, s)

        for j in range(cols):
            total = None
            for t in range(3):
                f = 3 * j + t
                block = lax.rem(ids[t, l, m * blocks + me * cols + j], blocks)
                lhs = source[block]
                if f < TA:
                    w = jnp.transpose(WA[q, :, :, f], (1, 0, 2, 3)).reshape(128, 128)
                else:
                    w = WB[q, :, :, f - TA].reshape(128, 128)
                d = jnp.dot(lhs, w, preferred_element_type=F32)
                total = d if total is None else total + d
            row = B[m, l : l + 1, j * 128 : (j + 1) * 128]
            value = jnp.clip(total + row, 0.0, 32.0).astype(BF16)
            if l == 0:
                O0[m, j] = value
            else:
                O1[m, :, j * 128 : (j + 1) * 128] = value
                acc[...] += value.astype(F32)

        @pl.when(m == me)
        def _():
            if l == 0:
                X1[mine] = O0[m]
            else:
                pltpu.make_async_copy(O1.at[me], out.at[:, mine_out], osem).start()

        @pl.when(m != me)
        def _():
            y_copy(l, m).start()

    def ring_steps(i, h):
        for stage, lags, direct in ((stage_b, LAGS_B, 4), (stage_a, LAGS_A, 2)):
            u = i - lags[h]
            k = u + HEAD
            valid = jnp.logical_and(u >= 0, k < chunks)
            if h >= direct:
                early = jnp.logical_and(u >= -direct, u < HEAD - direct)
                k = jnp.where(u < HEAD - direct, u + direct, k)
                valid = jnp.logical_or(valid, early)

            @pl.when(valid)
            def _():
                l, m = owner(k)
                stage(h, k, l * shards + m)

    done = max(LAGS_A[-1], LAGS_B[-1]) - HEAD

    def step(i, _):
        for h in range(7):
            ring_steps(i, h)

        first = i - done
        inner = jnp.logical_and(first >= 2, first <= shards)

        @pl.when(jnp.logical_or(first == 0, inner))
        def _():
            compute(0, first)

        opening = first == shards + 1

        def both(r, _):
            own_first = jnp.logical_and(opening, r == 0)
            compute(1, jnp.where(own_first, 1, first))
            return 0

        @pl.when(first > shards)
        def _():
            lax.fori_loop(0, jnp.where(opening, 2, 1), both, 0)

        return 0

    for k in range(HEAD):
        head(jnp.int32(k))
    lax.fori_loop(0, chunks + done, step, 0)

    part = jnp.sum(acc[...].T, axis=0, keepdims=True)
    RS[me] = part
    rs_copies = [
        remote(RS.at[me], RS.at[me], rss.at[i], rsr.at[me], mate(s)) for i, s in enumerate(mp_peers)
    ]
    for copy in rs_copies:
        copy.start()

    def drain(k, _):
        for copy in a_copies(k) + b_copies(k):
            copy().wait_send()
        return 0

    lax.fori_loop(0, chunks, drain, 0)
    for i, s in enumerate(mp_peers):
        remote(RS.at[s], RS.at[s], rss.at[i], rsr.at[s], mate(s)).wait_recv()
    row = jnp.sum(RS[...], axis=0) / neur
    means[...] = row
    G[b] = jnp.broadcast_to(jnp.sum(row, axis=1, keepdims=True), (1, 128))

    def tell(d, _):
        to = lax.rem(b + d, NX * NZ) * shards + me
        remote(G.at[b], G.at[b], gs, gr, to).start()
        return 0

    lax.fori_loop(1, NX * NZ, tell, 0)
    for l in range(layers):
        for i, s in enumerate(order):
            part_a(l, i, s).wait_send()
            part_b(l, i, s).wait_send()
        for s in mp_peers:
            y_copy(l, s).wait_send()
    for i, s in enumerate(order):
        bias_to(i, s).wait_send()
    for copy in rs_copies:
        copy.wait_send()
    for s in mp_peers:
        y_arrival(1, s)
    pltpu.make_async_copy(O1.at[me], out.at[:, mine_out], osem).wait()
    others = G.at[pl.ds(0, NX * NZ - 1)]
    pltpu.make_async_copy(others, others, gr).wait()
    grand[...] = jnp.sum(G[...], axis=0) / rows_all
    pltpu.make_async_copy(others, others, gs).wait()


def on_device(features, tiles, biases, in_block):
    layers, cb, fan, own_rows, side = tiles.shape
    rows = features.shape[0]
    shards = lax.axis_size("mp")
    groups = lax.axis_size("batch")
    per_chunk = cb // shards * fan
    chunks = layers * shards
    vmem = pl.BlockSpec(memory_space=pltpu.VMEM)
    hbm = pl.BlockSpec(memory_space=pltpu.HBM)
    dma = pltpu.SemaphoreType.DMA
    current, means, grand = pl.pallas_call(
        functools.partial(kernel, cb * shards * side, rows * groups),
        out_shape=(
            jax.ShapeDtypeStruct((rows, cb * side), BF16),
            jax.ShapeDtypeStruct((1, rows), F32),
            jax.ShapeDtypeStruct((1, 128), F32),
        ),
        in_specs=[hbm, hbm, hbm, hbm],
        out_specs=(vmem, vmem, vmem),
        scratch_shapes=[
            pltpu.VMEM((cb, rows, side), BF16),
            pltpu.VMEM((cb, rows, side), BF16),
            pltpu.VMEM((chunks, NZ, NX, TA, own_rows, side), BF16),
            pltpu.VMEM((chunks, NX, NZ, per_chunk - TA, own_rows, side), BF16),
            pltpu.VMEM((shards, layers, cb // shards * side), F32),
            pltpu.VMEM((shards, cb // shards, rows, side), BF16),
            pltpu.VMEM((shards, rows, cb // shards * side), BF16),
            pltpu.VMEM((rows, side), F32),
            pltpu.VMEM((shards, 1, 128), F32),
            pltpu.VMEM((NX * NZ, 1, 128), F32),
            pltpu.SMEM((fan, layers, shards * cb), jnp.int32),
            dma((layers, shards - 1, 2)),
            dma((chunks, 2)),
            dma((shards - 1,)),
            dma((shards,)),
            dma((chunks, 12)),
            dma((chunks, 12)),
            dma((chunks, 12)),
            dma((chunks, 12)),
            dma((layers, shards)),
            dma((layers, shards)),
            dma((shards - 1,)),
            dma((shards,)),
            dma,
            dma,
            dma,
            dma,
            dma,
        ],
        compiler_params=pltpu.CompilerParams(
            collective_id=0, has_side_effects=True, vmem_limit_bytes=48 * 1024 * 1024
        ),
    )(
        *(
            pltpu.with_memory_space_constraint(v, pltpu.HBM)
            for v in (
                jnp.transpose(in_block, (2, 0, 1)),
                features,
                tiles.reshape(layers, shards, per_chunk, own_rows, side),
                biases,
            )
        )
    )
    return current, means.reshape(rows), grand[0, 0]


def solution(mesh):
    placed = (P("batch", "mp"), P(None, "mp", None, "batch", None), P(None, "mp"), P())
    return jax.shard_map(
        on_device,
        mesh=mesh,
        in_specs=placed,
        out_specs=(P("batch", "mp"), P("batch"), P()),
        check_vma=False,
    )
```

```python
import functools

import jax
import jax.numpy as jnp
from jax import lax
from jax.experimental import pallas as pl
from jax.experimental.pallas import tpu as pltpu
from jax.sharding import PartitionSpec as P

NX, NZ = 4, 8
NY, NC = 4, 2
TA = 10
LAGS_A = (0, 1, 2, 3, 4, 5, 6)
LAGS_B = (0, 1, 2, 3, 4, 5, 6)
SLOTS = 5
F32 = jnp.float32
BF16 = jnp.bfloat16


def kernel(
    neur, rows_all,
    ib, feat, tiles, bias,
    out, means, grand,
    X0, X1, WA, WB, B, O0, O1, acc, RS, G, ids,
    p0s, p0r, pbs, pbr, sA, rA, sB, rB, ys, yr, rss, rsr, gs, gr, fsem, isem, osem,
):
    layers = tiles.shape[0]
    shards = tiles.shape[1]
    per_chunk = tiles.shape[2]
    cols = per_chunk // 3
    blocks = cols * shards
    chunks = layers * shards
    b = lax.axis_index("batch")
    me = lax.axis_index("mp")
    x, z = b // NZ, b % NZ
    y, c = me // NC, me % NC
    xr, xl = (x + 1) % NX, (x + NX - 1) % NX

    def zat(d):
        return (z + d + NZ) % NZ

    def device(xx, zz, s):
        return (xx * NZ + zz) * shards + s

    near = {d: zat(d) for d in range(-3, 4)}
    right, left = device(xr, z, me), device(xl, z, me)
    up, down = device(x, near[1], me), device(x, near[-1], me)

    def peer(dy, dc):
        return lax.rem(y + dy, NY) * NC + lax.rem(c + dc, NC)

    def mate(s):
        return device(x, z, s)

    offsets = [(2, 0), (2, 1), (1, 0), (3, 0), (1, 1), (3, 1), (0, 1)]
    mp_peers = [peer(dy, dc) for dy, dc in offsets]

    def remote(src, dst, ss, rs, dev):
        return pltpu.make_async_remote_copy(
            src_ref=src,
            dst_ref=dst,
            send_sem=ss,
            recv_sem=rs,
            device_id=dev,
            device_id_type=pl.DeviceIdType.LOGICAL,
        )

    def load(j, _):
        at_j = pl.ds(pl.multiple_of(j * 128, 128), 128)
        pltpu.make_async_copy(feat.at[:, at_j], X0.at[j], fsem).start()
        return 0

    barrier = pltpu.get_barrier_semaphore()
    greeted = [mate(s) for s in mp_peers] + [right, left, up, down]
    for dev in greeted:
        pl.semaphore_signal(
            barrier, inc=1, device_id=dev, device_id_type=pl.DeviceIdType.LOGICAL
        )
    own = []
    for l in range(layers):
        q = l * shards + me
        own.append(
            pltpu.make_async_copy(tiles.at[l, me, 0:TA], WA.at[q, z, x], p0r.at[q, 0])
        )
        own.append(
            pltpu.make_async_copy(tiles.at[l, me, TA:per_chunk], WB.at[q, x, z], p0r.at[q, 1])
        )
    own.append(
        pltpu.make_async_copy(
            bias.at[:, pl.ds(pl.multiple_of(me * cols * 128, 128), cols * 128)],
            B.at[me],
            pbr.at[me],
        )
    )
    for copy in own:
        copy.start()
    pltpu.make_async_copy(ib, ids, isem).start()
    lax.fori_loop(0, blocks, load, 0)
    pl.semaphore_wait(barrier, len(greeted))

    def part_a(l, i, s):
        q = l * shards + me
        return remote(
            tiles.at[l, s, 0:TA], WA.at[q, z, x], p0s.at[l, i, 0], p0r.at[q, 0], mate(s)
        )

    def part_b(l, i, s):
        q = l * shards + me
        return remote(
            tiles.at[l, s, TA:per_chunk], WB.at[q, x, z], p0s.at[l, i, 1], p0r.at[q, 1], mate(s)
        )

    def bias_to(i, s):
        cut = pl.ds(pl.multiple_of(s * cols * 128, 128), cols * 128)
        return remote(bias.at[:, cut], B.at[me], pbs.at[i], pbr.at[me], mate(s))

    order = [peer(NY - dy, dc) for dy, dc in offsets]
    for l in range(layers):
        for i in range(shards - 1):
            part_a(l, i, order[i]).start()
            part_b(l, i, order[i]).start()
        if l == 0:
            for i, s in enumerate(order):
                bias_to(i, s).start()

    acc[...] = jnp.zeros_like(acc)

    def owner(k):
        tail = k >= shards + 1
        l = jnp.where(jnp.logical_or(k == 1, tail), 1, 0)
        n = jnp.where(k < 2, shards - 1, jnp.where(tail, k - (shards + 1), k - 2))
        dy = jnp.where(n < 2, 2, jnp.where(n < 6, 1 + 2 * lax.rem(n, 2), 0))
        dc = jnp.where(n < 2, n, jnp.where(n < 6, lax.div(n - 2, 2), 7 - n))
        return l, peer(dy, dc)

    def a_copies(q, k):
        slot = lax.rem(k, SLOTS)

        def go(ref, i, dev):
            return lambda: remote(ref, ref, sA.at[slot, i], rA.at[slot, i], dev)

        half, cut = NX // 2, TA // 2
        return [
            go(WA.at[q, z, x], 0, right),
            go(WA.at[q, z, x], 1, left),
            go(WA.at[q, z, xl, 0:cut], 2, right),
            go(WA.at[q, z, xr, cut:TA], 3, left),
            go(WA.at[q, z], 4, up),
            go(WA.at[q, z], 5, down),
            go(WA.at[q, near[-1]], 6, up),
            go(WA.at[q, near[1]], 7, down),
            go(WA.at[q, near[-2]], 8, up),
            go(WA.at[q, near[2]], 9, down),
            go(WA.at[q, near[-3], 0:half], 10, up),
            go(WA.at[q, near[3], half:NX], 11, down),
        ]

    def b_copies(q, k):
        slot = lax.rem(k, SLOTS)

        def go(ref, i, dev):
            return lambda: remote(ref, ref, sB.at[slot, i], rB.at[slot, i], dev)

        tb = per_chunk - TA
        half, cut = NZ // 2, tb // 2
        return [
            go(WB.at[q, x, z], 0, up),
            go(WB.at[q, x, z], 1, down),
            go(WB.at[q, x, near[-1]], 2, up),
            go(WB.at[q, x, near[1]], 3, down),
            go(WB.at[q, x, near[-2]], 4, up),
            go(WB.at[q, x, near[2]], 5, down),
            go(WB.at[q, x, near[-3], 0:cut], 6, up),
            go(WB.at[q, x, near[3], cut:tb], 7, down),
            go(WB.at[q, x], 8, right),
            go(WB.at[q, x], 9, left),
            go(WB.at[q, xl, 0:half], 10, right),
            go(WB.at[q, xr, half:NZ], 11, left),
        ]

    def stage_a(h, k, q):
        copies = a_copies(q, k)

        def forward(needs, starts):
            for n in needs:
                copies[n]().wait_recv()
            if starts:

                @pl.when(k >= SLOTS)
                def _():
                    for n in starts:
                        copies[n]().wait_send()

            for n in starts:
                copies[n]().start()

        if h == 0:
            pltpu.make_async_copy(WA.at[q, z, x], WA.at[q, z, x], p0r.at[q, 0]).wait()
            forward((), (0, 1))
        elif h == 1:
            forward((0,), (2,))
            forward((1,), (3,))
        elif h == 2:
            forward((2, 3), (4, 5))
        elif h < 6:
            forward((2 * h - 2,), (2 * h,))
            forward((2 * h - 1,), (2 * h + 1,))
        else:
            forward((10, 11), ())

    def stage_b(h, k, q):
        copies = b_copies(q, k)

        def forward(needs, starts):
            for n in needs:
                copies[n]().wait_recv()
            if starts:

                @pl.when(k >= SLOTS)
                def _():
                    for n in starts:
                        copies[n]().wait_send()

            for n in starts:
                copies[n]().start()

        if h == 0:
            pltpu.make_async_copy(WB.at[q, x, z], WB.at[q, x, z], p0r.at[q, 1]).wait()
            forward((), (0, 1))
        elif h == 4:
            forward((6, 7), (8, 9))
        elif h < 6:
            forward((2 * h - 2,), (2 * h,))
            forward((2 * h - 1,), (2 * h + 1,))
        else:
            forward((10, 11), ())

    mine = pl.ds(me * cols, cols)
    mine_out = pl.ds(pl.multiple_of(me * cols * 128, 128), cols * 128)

    def y_copy(l, m):
        if l == 0:
            src, dst = O0.at[m], X1.at[mine]
        else:
            src, dst = O1.at[m], out.at[:, mine_out]
        return remote(src, dst, ys.at[l, m], yr.at[l, me], mate(m))

    def y_arrival(l, s):
        if l == 0:
            src, dst = O0.at[s], X1.at[pl.ds(s * cols, cols)]
        else:
            cut = pl.ds(pl.multiple_of(s * cols * 128, 128), cols * 128)
            src, dst = O1.at[s], out.at[:, cut]
        remote(src, dst, ys.at[l, s], yr.at[l, s], mate(s)).wait_recv()

    def compute(l, k):
        _, m = owner(k)
        q = l * shards + m
        source = X0 if l == 0 else X1
        if l == 0:

            @pl.when(k == 0)
            def _():
                pltpu.make_async_copy(X0, X0, fsem).wait()
                pltpu.make_async_copy(ib, ids, isem).wait()

            pltpu.make_async_copy(B.at[m], B.at[m], pbr.at[m]).wait()
        else:

            @pl.when(k == 1)
            def _():
                for s in mp_peers:
                    y_arrival(0, s)

        for j in range(cols):
            total = None
            for t in range(3):
                f = 3 * j + t
                block = lax.rem(ids[t, l, m * blocks + me * cols + j], blocks)
                lhs = source[block]
                if f < TA:
                    w = jnp.transpose(WA[q, :, :, f], (1, 0, 2, 3)).reshape(128, 128)
                else:
                    w = WB[q, :, :, f - TA].reshape(128, 128)
                d = jnp.dot(lhs, w, preferred_element_type=F32)
                total = d if total is None else total + d
            row = B[m, l : l + 1, j * 128 : (j + 1) * 128]
            value = jnp.clip(total + row, 0.0, 32.0).astype(BF16)
            if l == 0:
                O0[m, j] = value
            else:
                O1[m, :, j * 128 : (j + 1) * 128] = value
                acc[...] += value.astype(F32)

        @pl.when(m == me)
        def _():
            if l == 0:
                X1[mine] = O0[m]
            else:
                pltpu.make_async_copy(O1.at[me], out.at[:, mine_out], osem).start()

        @pl.when(m != me)
        def _():
            y_copy(l, m).start()

    def ring_steps(i, h):
        for stage, lags in ((stage_b, LAGS_B), (stage_a, LAGS_A)):
            k = i - lags[h]

            @pl.when(jnp.logical_and(k >= 0, k < chunks))
            def _():
                l, m = owner(k)
                stage(h, k, l * shards + m)

    done = max(LAGS_A[-1], LAGS_B[-1])

    def step(i, _):
        for h in range(7):
            ring_steps(i, h)

        first = i - done
        inner = jnp.logical_and(first >= 2, first <= shards)

        @pl.when(jnp.logical_or(first == 0, inner))
        def _():
            compute(0, first)

        opening = first == shards + 1

        def both(r, _):
            own_first = jnp.logical_and(opening, r == 0)
            compute(1, jnp.where(own_first, 1, first))
            return 0

        @pl.when(first > shards)
        def _():
            lax.fori_loop(0, jnp.where(opening, 2, 1), both, 0)

        return 0

    lax.fori_loop(0, chunks + done, step, 0)

    part = jnp.sum(acc[...].T, axis=0, keepdims=True)
    RS[me] = part
    rs_copies = [
        remote(RS.at[me], RS.at[me], rss.at[i], rsr.at[me], mate(s)) for i, s in enumerate(mp_peers)
    ]
    for copy in rs_copies:
        copy.start()

    def drain(k, _):
        for copy in a_copies(k, k) + b_copies(k, k):
            copy().wait_send()
        return 0

    lax.fori_loop(0, SLOTS, drain, 0)
    for i, s in enumerate(mp_peers):
        remote(RS.at[s], RS.at[s], rss.at[i], rsr.at[s], mate(s)).wait_recv()
    row = jnp.sum(RS[...], axis=0) / neur
    means[...] = row
    G[b] = jnp.broadcast_to(jnp.sum(row, axis=1, keepdims=True), (1, 128))

    def tell(d, _):
        to = lax.rem(b + d, NX * NZ) * shards + me
        remote(G.at[b], G.at[b], gs, gr, to).start()
        return 0

    lax.fori_loop(1, NX * NZ, tell, 0)
    for l in range(layers):
        for i, s in enumerate(order):
            part_a(l, i, s).wait_send()
            part_b(l, i, s).wait_send()
        for s in mp_peers:
            y_copy(l, s).wait_send()
    for i, s in enumerate(order):
        bias_to(i, s).wait_send()
    for copy in rs_copies:
        copy.wait_send()
    for s in mp_peers:
        y_arrival(1, s)
    pltpu.make_async_copy(O1.at[me], out.at[:, mine_out], osem).wait()
    others = G.at[pl.ds(0, NX * NZ - 1)]
    pltpu.make_async_copy(others, others, gr).wait()
    grand[...] = jnp.sum(G[...], axis=0) / rows_all
    pltpu.make_async_copy(others, others, gs).wait()


def on_device(features, tiles, biases, in_block):
    layers, cb, fan, own_rows, side = tiles.shape
    rows = features.shape[0]
    shards = lax.axis_size("mp")
    groups = lax.axis_size("batch")
    per_chunk = cb // shards * fan
    chunks = layers * shards
    vmem = pl.BlockSpec(memory_space=pltpu.VMEM)
    hbm = pl.BlockSpec(memory_space=pltpu.HBM)
    dma = pltpu.SemaphoreType.DMA
    current, means, grand = pl.pallas_call(
        functools.partial(kernel, cb * shards * side, rows * groups),
        out_shape=(
            jax.ShapeDtypeStruct((rows, cb * side), BF16),
            jax.ShapeDtypeStruct((1, rows), F32),
            jax.ShapeDtypeStruct((1, 128), F32),
        ),
        in_specs=[hbm, hbm, hbm, hbm],
        out_specs=(vmem, vmem, vmem),
        scratch_shapes=[
            pltpu.VMEM((cb, rows, side), BF16),
            pltpu.VMEM((cb, rows, side), BF16),
            pltpu.VMEM((chunks, NZ, NX, TA, own_rows, side), BF16),
            pltpu.VMEM((chunks, NX, NZ, per_chunk - TA, own_rows, side), BF16),
            pltpu.VMEM((shards, layers, cb // shards * side), F32),
            pltpu.VMEM((shards, cb // shards, rows, side), BF16),
            pltpu.VMEM((shards, rows, cb // shards * side), BF16),
            pltpu.VMEM((rows, side), F32),
            pltpu.VMEM((shards, 1, 128), F32),
            pltpu.VMEM((NX * NZ, 1, 128), F32),
            pltpu.SMEM((fan, layers, shards * cb), jnp.int32),
            dma((layers, shards - 1, 2)),
            dma((chunks, 2)),
            dma((shards - 1,)),
            dma((shards,)),
            dma((SLOTS, 12)),
            dma((SLOTS, 12)),
            dma((SLOTS, 12)),
            dma((SLOTS, 12)),
            dma((layers, shards)),
            dma((layers, shards)),
            dma((shards - 1,)),
            dma((shards,)),
            dma,
            dma,
            dma,
            dma,
            dma,
        ],
        compiler_params=pltpu.CompilerParams(
            collective_id=0, has_side_effects=True, vmem_limit_bytes=48 * 1024 * 1024
        ),
    )(
        *(
            pltpu.with_memory_space_constraint(v, pltpu.HBM)
            for v in (
                jnp.transpose(in_block, (2, 0, 1)),
                features,
                tiles.reshape(layers, shards, per_chunk, own_rows, side),
                biases,
            )
        )
    )
    return current, means.reshape(rows), grand[0, 0]


def solution(mesh):
    placed = (P("batch", "mp"), P(None, "mp", None, "batch", None), P(None, "mp"), P())
    return jax.shard_map(
        on_device,
        mesh=mesh,
        in_specs=placed,
        out_specs=(P("batch", "mp"), P("batch"), P()),
        check_vma=False,
    )
```

```python
import functools

import jax
import jax.numpy as jnp
from jax import lax
from jax.experimental import pallas as pl
from jax.experimental.pallas import tpu as pltpu
from jax.sharding import PartitionSpec as P

NX, NZ = 4, 8
NY, NC = 4, 2
TA = 10
LAGS_A = (0, 1, 2, 3, 4, 5, 6)
LAGS_B = (0, 1, 2, 3, 4, 5, 6)
SLOTS = 4
F32 = jnp.float32
BF16 = jnp.bfloat16


def kernel(
    neur, rows_all,
    ib, feat, tiles, bias,
    out, means, grand,
    X0, X1, WA, WB, B, O0, O1, acc, RS, G, ids,
    p0s, p0r, pbs, pbr, sA, rA, sB, rB, ys, yr, rss, rsr, gs, gr, fsem, isem, osem,
):
    layers = tiles.shape[0]
    shards = tiles.shape[1]
    per_chunk = tiles.shape[2]
    cols = per_chunk // 3
    blocks = cols * shards
    chunks = layers * shards
    b = lax.axis_index("batch")
    me = lax.axis_index("mp")
    x, z = b // NZ, b % NZ
    y, c = me // NC, me % NC
    xr, xl = (x + 1) % NX, (x + NX - 1) % NX

    def zat(d):
        return (z + d + NZ) % NZ

    def device(xx, zz, s):
        return (xx * NZ + zz) * shards + s

    near = {d: zat(d) for d in range(-3, 4)}
    right, left = device(xr, z, me), device(xl, z, me)
    up, down = device(x, near[1], me), device(x, near[-1], me)

    def peer(dy, dc):
        return lax.rem(y + dy, NY) * NC + lax.rem(c + dc, NC)

    def mate(s):
        return device(x, z, s)

    offsets = [(2, 0), (2, 1), (1, 0), (3, 0), (1, 1), (3, 1), (0, 1)]
    mp_peers = [peer(dy, dc) for dy, dc in offsets]

    def remote(src, dst, ss, rs, dev):
        return pltpu.make_async_remote_copy(
            src_ref=src,
            dst_ref=dst,
            send_sem=ss,
            recv_sem=rs,
            device_id=dev,
            device_id_type=pl.DeviceIdType.LOGICAL,
        )

    def load(j, _):
        at_j = pl.ds(pl.multiple_of(j * 128, 128), 128)
        pltpu.make_async_copy(feat.at[:, at_j], X0.at[j], fsem).start()
        return 0

    barrier = pltpu.get_barrier_semaphore()
    greeted = [mate(s) for s in mp_peers] + [right, left, up, down]
    for dev in greeted:
        pl.semaphore_signal(
            barrier, inc=1, device_id=dev, device_id_type=pl.DeviceIdType.LOGICAL
        )
    own = []
    for l in range(layers):
        q = l * shards + me
        own.append(
            pltpu.make_async_copy(tiles.at[l, me, 0:TA], WA.at[q, z, x], p0r.at[q, 0])
        )
        own.append(
            pltpu.make_async_copy(tiles.at[l, me, TA:per_chunk], WB.at[q, x, z], p0r.at[q, 1])
        )
    own.append(
        pltpu.make_async_copy(
            bias.at[:, pl.ds(pl.multiple_of(me * cols * 128, 128), cols * 128)],
            B.at[me],
            pbr.at[me],
        )
    )
    for copy in own:
        copy.start()
    pltpu.make_async_copy(ib, ids, isem).start()
    lax.fori_loop(0, blocks, load, 0)
    pl.semaphore_wait(barrier, len(greeted))

    def part_a(l, i, s):
        q = l * shards + me
        return remote(
            tiles.at[l, s, 0:TA], WA.at[q, z, x], p0s, p0r.at[q, 0], mate(s)
        )

    def part_b(l, i, s):
        q = l * shards + me
        return remote(
            tiles.at[l, s, TA:per_chunk], WB.at[q, x, z], p0s, p0r.at[q, 1], mate(s)
        )

    def bias_to(i, s):
        cut = pl.ds(pl.multiple_of(s * cols * 128, 128), cols * 128)
        return remote(bias.at[:, cut], B.at[me], pbs, pbr.at[me], mate(s))

    order = [peer(NY - dy, dc) for dy, dc in offsets]
    for l in range(layers):
        for i in range(shards - 1):
            part_a(l, i, order[i]).start()
            part_b(l, i, order[i]).start()
        if l == 0:
            for i, s in enumerate(order):
                bias_to(i, s).start()

    acc[...] = jnp.zeros_like(acc)

    def owner(k):
        tail = k >= shards + 1
        l = jnp.where(jnp.logical_or(k == 1, tail), 1, 0)
        n = jnp.where(k < 2, shards - 1, jnp.where(tail, k - (shards + 1), k - 2))
        dy = jnp.where(n < 2, 2, jnp.where(n < 6, 1 + 2 * lax.rem(n, 2), 0))
        dc = jnp.where(n < 2, n, jnp.where(n < 6, lax.div(n - 2, 2), 7 - n))
        return l, peer(dy, dc)

    def a_copies(q, k):
        slot = lax.rem(k, SLOTS)

        def go(ref, i, dev):
            return lambda: remote(ref, ref, sA.at[slot, i], rA.at[slot, i], dev)

        half, cut = NX // 2, TA // 2
        return [
            go(WA.at[q, z, x], 0, right),
            go(WA.at[q, z, x], 1, left),
            go(WA.at[q, z, xl, 0:cut], 2, right),
            go(WA.at[q, z, xr, cut:TA], 3, left),
            go(WA.at[q, z], 4, up),
            go(WA.at[q, z], 5, down),
            go(WA.at[q, near[-1]], 6, up),
            go(WA.at[q, near[1]], 7, down),
            go(WA.at[q, near[-2]], 8, up),
            go(WA.at[q, near[2]], 9, down),
            go(WA.at[q, near[-3], 0:half], 10, up),
            go(WA.at[q, near[3], half:NX], 11, down),
        ]

    def b_copies(q, k):
        slot = lax.rem(k, SLOTS)

        def go(ref, i, dev):
            return lambda: remote(ref, ref, sB.at[slot, i], rB.at[slot, i], dev)

        tb = per_chunk - TA
        half, cut = NZ // 2, tb // 2
        return [
            go(WB.at[q, x, z], 0, up),
            go(WB.at[q, x, z], 1, down),
            go(WB.at[q, x, near[-1]], 2, up),
            go(WB.at[q, x, near[1]], 3, down),
            go(WB.at[q, x, near[-2]], 4, up),
            go(WB.at[q, x, near[2]], 5, down),
            go(WB.at[q, x, near[-3], 0:cut], 6, up),
            go(WB.at[q, x, near[3], cut:tb], 7, down),
            go(WB.at[q, x], 8, right),
            go(WB.at[q, x], 9, left),
            go(WB.at[q, xl, 0:half], 10, right),
            go(WB.at[q, xr, half:NZ], 11, left),
        ]

    def stage_a(h, k, q):
        copies = a_copies(q, k)

        def forward(needs, starts):
            for n in needs:
                copies[n]().wait_recv()
            if starts:

                @pl.when(k >= SLOTS)
                def _():
                    for n in starts:
                        copies[n]().wait_send()

            for n in starts:
                copies[n]().start()

        if h == 0:
            pltpu.make_async_copy(WA.at[q, z, x], WA.at[q, z, x], p0r.at[q, 0]).wait()
            forward((), (0, 1))
        elif h == 1:
            forward((0,), (2,))
            forward((1,), (3,))
        elif h == 2:
            forward((2, 3), (4, 5))
        elif h < 6:
            forward((2 * h - 2,), (2 * h,))
            forward((2 * h - 1,), (2 * h + 1,))
        else:
            forward((10, 11), ())

    def stage_b(h, k, q):
        copies = b_copies(q, k)

        def forward(needs, starts):
            for n in needs:
                copies[n]().wait_recv()
            if starts:

                @pl.when(k >= SLOTS)
                def _():
                    for n in starts:
                        copies[n]().wait_send()

            for n in starts:
                copies[n]().start()

        if h == 0:
            pltpu.make_async_copy(WB.at[q, x, z], WB.at[q, x, z], p0r.at[q, 1]).wait()
            forward((), (0, 1))
        elif h == 4:
            forward((6, 7), (8, 9))
        elif h < 6:
            forward((2 * h - 2,), (2 * h,))
            forward((2 * h - 1,), (2 * h + 1,))
        else:
            forward((10, 11), ())

    mine = pl.ds(me * cols, cols)
    mine_out = pl.ds(pl.multiple_of(me * cols * 128, 128), cols * 128)

    def y_copy(l, m):
        if l == 0:
            src, dst = O0.at[m], X1.at[mine]
        else:
            src, dst = O1.at[m], out.at[:, mine_out]
        return remote(src, dst, ys.at[l], yr.at[l, me], mate(m))

    def y_arrival(l, s):
        if l == 0:
            src, dst = O0.at[s], X1.at[pl.ds(s * cols, cols)]
        else:
            cut = pl.ds(pl.multiple_of(s * cols * 128, 128), cols * 128)
            src, dst = O1.at[s], out.at[:, cut]
        remote(src, dst, ys.at[l], yr.at[l, s], mate(s)).wait_recv()

    def compute(l, k):
        _, m = owner(k)
        q = l * shards + m
        source = X0 if l == 0 else X1
        if l == 0:

            @pl.when(k == 0)
            def _():
                pltpu.make_async_copy(X0, X0, fsem).wait()
                pltpu.make_async_copy(ib, ids, isem).wait()

            pltpu.make_async_copy(B.at[m], B.at[m], pbr.at[m]).wait()
        else:

            @pl.when(k == 1)
            def _():
                for s in mp_peers:
                    y_arrival(0, s)

        for j in range(cols):
            total = None
            for t in range(3):
                f = 3 * j + t
                block = lax.rem(ids[t, l, m * blocks + me * cols + j], blocks)
                lhs = source[block]
                if f < TA:
                    w = jnp.transpose(WA[q, :, :, f], (1, 0, 2, 3)).reshape(128, 128)
                else:
                    w = WB[q, :, :, f - TA].reshape(128, 128)
                d = jnp.dot(lhs, w, preferred_element_type=F32)
                total = d if total is None else total + d
            row = B[m, l : l + 1, j * 128 : (j + 1) * 128]
            value = jnp.clip(total + row, 0.0, 32.0).astype(BF16)
            if l == 0:
                O0[m, j] = value
            else:
                O1[m, :, j * 128 : (j + 1) * 128] = value
                acc[...] += value.astype(F32)

        @pl.when(m == me)
        def _():
            if l == 0:
                X1[mine] = O0[m]
            else:
                pltpu.make_async_copy(O1.at[me], out.at[:, mine_out], osem).start()

        @pl.when(m != me)
        def _():
            y_copy(l, m).start()

    def ring_steps(i, h):
        for stage, lags in ((stage_b, LAGS_B), (stage_a, LAGS_A)):
            k = i - lags[h]

            @pl.when(jnp.logical_and(k >= 0, k < chunks))
            def _():
                l, m = owner(k)
                stage(h, k, l * shards + m)

    done = max(LAGS_A[-1], LAGS_B[-1])

    def step(i, _):
        for h in range(7):
            ring_steps(i, h)

        first = i - done
        inner = jnp.logical_and(first >= 2, first <= shards)

        @pl.when(jnp.logical_or(first == 0, inner))
        def _():
            compute(0, first)

        opening = first == shards + 1

        def both(r, _):
            own_first = jnp.logical_and(opening, r == 0)
            compute(1, jnp.where(own_first, 1, first))
            return 0

        @pl.when(first > shards)
        def _():
            lax.fori_loop(0, jnp.where(opening, 2, 1), both, 0)

        return 0

    lax.fori_loop(0, chunks + done, step, 0)

    part = jnp.sum(acc[...].T, axis=0, keepdims=True)
    RS[me] = part
    rs_copies = [
        remote(RS.at[me], RS.at[me], rss, rsr.at[me], mate(s)) for i, s in enumerate(mp_peers)
    ]
    for copy in rs_copies:
        copy.start()

    def drain(k, _):
        for copy in a_copies(k, k) + b_copies(k, k):
            copy().wait_send()
        return 0

    lax.fori_loop(0, SLOTS, drain, 0)
    for i, s in enumerate(mp_peers):
        remote(RS.at[s], RS.at[s], rss, rsr.at[s], mate(s)).wait_recv()
    row = jnp.sum(RS[...], axis=0) / neur
    means[...] = row
    G[b] = jnp.broadcast_to(jnp.sum(row, axis=1, keepdims=True), (1, 128))

    def tell(d, _):
        to = lax.rem(b + d, NX * NZ) * shards + me
        remote(G.at[b], G.at[b], gs, gr, to).start()
        return 0

    lax.fori_loop(1, NX * NZ, tell, 0)
    peers = pl.ds(0, shards - 1)
    sent = (
        (tiles.at[:, peers], p0s),
        (bias.at[:, pl.ds(0, (shards - 1) * cols * 128)], pbs),
        (O0.at[peers], ys.at[0]),
        (O1.at[peers], ys.at[1]),
        (RS.at[peers], rss),
    )
    for ref, sem in sent:
        pltpu.make_async_copy(ref, ref, sem).wait()
    for s in mp_peers:
        y_arrival(1, s)
    pltpu.make_async_copy(O1.at[me], out.at[:, mine_out], osem).wait()
    others = G.at[pl.ds(0, NX * NZ - 1)]
    pltpu.make_async_copy(others, others, gr).wait()
    grand[...] = jnp.sum(G[...], axis=0) / rows_all
    pltpu.make_async_copy(others, others, gs).wait()


def on_device(features, tiles, biases, in_block):
    layers, cb, fan, own_rows, side = tiles.shape
    rows = features.shape[0]
    shards = lax.axis_size("mp")
    groups = lax.axis_size("batch")
    per_chunk = cb // shards * fan
    chunks = layers * shards
    vmem = pl.BlockSpec(memory_space=pltpu.VMEM)
    hbm = pl.BlockSpec(memory_space=pltpu.HBM)
    dma = pltpu.SemaphoreType.DMA
    current, means, grand = pl.pallas_call(
        functools.partial(kernel, cb * shards * side, rows * groups),
        out_shape=(
            jax.ShapeDtypeStruct((rows, cb * side), BF16),
            jax.ShapeDtypeStruct((1, rows), F32),
            jax.ShapeDtypeStruct((1, 128), F32),
        ),
        in_specs=[hbm, hbm, hbm, hbm],
        out_specs=(vmem, vmem, vmem),
        scratch_shapes=[
            pltpu.VMEM((cb, rows, side), BF16),
            pltpu.VMEM((cb, rows, side), BF16),
            pltpu.VMEM((chunks, NZ, NX, TA, own_rows, side), BF16),
            pltpu.VMEM((chunks, NX, NZ, per_chunk - TA, own_rows, side), BF16),
            pltpu.VMEM((shards, layers, cb // shards * side), F32),
            pltpu.VMEM((shards, cb // shards, rows, side), BF16),
            pltpu.VMEM((shards, rows, cb // shards * side), BF16),
            pltpu.VMEM((rows, side), F32),
            pltpu.VMEM((shards, 1, 128), F32),
            pltpu.VMEM((NX * NZ, 1, 128), F32),
            pltpu.SMEM((fan, layers, shards * cb), jnp.int32),
            dma,
            dma((chunks, 2)),
            dma,
            dma((shards,)),
            dma((SLOTS, 12)),
            dma((SLOTS, 12)),
            dma((SLOTS, 12)),
            dma((SLOTS, 12)),
            dma((layers,)),
            dma((layers, shards)),
            dma,
            dma((shards,)),
            dma,
            dma,
            dma,
            dma,
            dma,
        ],
        compiler_params=pltpu.CompilerParams(
            collective_id=0, has_side_effects=True, vmem_limit_bytes=48 * 1024 * 1024
        ),
    )(
        *(
            pltpu.with_memory_space_constraint(v, pltpu.HBM)
            for v in (
                jnp.transpose(in_block, (2, 0, 1)),
                features,
                tiles.reshape(layers, shards, per_chunk, own_rows, side),
                biases,
            )
        )
    )
    return current, means.reshape(rows), grand[0, 0]


def solution(mesh):
    placed = (P("batch", "mp"), P(None, "mp", None, "batch", None), P(None, "mp"), P())
    return jax.shard_map(
        on_device,
        mesh=mesh,
        in_specs=placed,
        out_specs=(P("batch", "mp"), P("batch"), P()),
        check_vma=False,
    )
```
